32 devices in a mesh: vrow: 8 (over z, y), vcol: 4 (over x, core).
Axes of the slice: x: 2, y: 2, z: 4, core: 2. Of those that a mesh axis runs over, the one named last changes fastest.
Arguments:
- policy_hidden: bfloat16 [1024, 3584], P(None, 'vcol'), may hold values from -400 to 400
- ref_hidden: bfloat16 [1024, 3584], P(None, 'vcol'), may hold values from -400 to 400
- mix_num: int32 [1024], replicated, may hold values from 0 to 16, as said below
- mix_den: int32 [1024], replicated, may hold values from 2 to 16
- policy_unembed: bfloat16 [3584, 16384], P(None, ('vrow', 'vcol')), may hold values from -0.09375 to 0.09375
- ref_unembed: bfloat16 [3584, 16384], P(None, ('vrow', 'vcol')), may hold values from -0.09375 to 0.09375
Outputs:
- mix_logprobs: float32 [1024, 16384], P(None, ('vrow', 'vcol'))
The draws below stay inside these ranges and needn't reach their ends.
Inputs may be any that keep to these rules, and one draw needn't show every extreme that they name: Each sequence's mix_num is at most its mix_den.
All inputs are finite; a program needn't handle non-finite values.
Results may differ from the reference program's by a relative error of at most 0.0003.
Values may be sent and summed in bfloat16 or wider, within the bound.
No kernel may reach another device: no remote copies, remote signals or barrier semaphores. Data moves between devices by JAX's collectives and lax.ppermute only.
A program may use at most 64 MiB of HBM per device.

```python
import jax
import jax.numpy as jnp

D = 3584
B = 1024
VOCAB = 16384


def weight_pair(key):
    base = jax.random.fold_in(key, 7)
    first, second = jax.random.split(base)
    denom = jax.random.randint(first, (B,), 2, 17)
    numer = jax.random.randint(second, (B,), 0, 17) % (denom + 1)
    return (numer.astype(jnp.int32), denom.astype(jnp.int32))


def draw_mix_num(key, part):
    return weight_pair(key)[0]


def draw_mix_den(key, part):
    return weight_pair(key)[1]


def hidden_law(key, salt):
    base = jax.random.fold_in(key, salt)
    first = jax.random.fold_in(base, 0)
    values = 3.0 * jax.random.normal(first, (B, D), jnp.float32)
    return jnp.clip(values, -400.0, 400.0).astype(jnp.bfloat16)


def draw_policy_hidden(key, part):
    return hidden_law(key, 11)


def draw_ref_hidden(key, part):
    return hidden_law(key, 13)


def block_scale(own_key, shape, cuts, least, largest):
    def one(dim, shards_of):
        heights = jax.random.uniform(jax.random.fold_in(jax.random.fold_in(own_key, 6), dim), (shards_of,), jnp.float32, least / len(cuts), largest / len(cuts))
        return jnp.repeat(jnp.exp(heights), shape[dim] // shards_of).reshape((-1,) + (1,) * (len(shape) - dim - 1))

    level = one(*cuts[0])
    for cut in cuts[1:]:
        level = level * one(*cut)
    return level


def gaussian(rng, dims, deviation, bound, shards=(), held_as=jnp.bfloat16):
    level = block_scale(rng, dims, shards, -0.22, 0.18) if shards else 1.0
    result = jax.random.normal(rng, dims, jnp.float32) * deviation * level
    return jnp.minimum(jnp.maximum(result, -bound), bound).astype(held_as)


def setup_inputs(seed: int = 0) -> dict:
    key_of = jax.random.split(jax.random.key(seed), 7)
    return {
        "policy_hidden": draw_policy_hidden(jax.random.fold_in(key_of[6], 71), 0),
        "ref_hidden": draw_ref_hidden(jax.random.fold_in(key_of[6], 71), 0),
        "mix_num": draw_mix_num(jax.random.fold_in(key_of[6], 71), 0),
        "mix_den": draw_mix_den(jax.random.fold_in(key_of[6], 71), 0),
        "policy_unembed": gaussian(key_of[4], (D, VOCAB), D ** -0.5, 0.09375, ((1, 32),)),
        "ref_unembed": gaussian(key_of[5], (D, VOCAB), D ** -0.5, 0.09375, ((1, 32),)),
    }


def reference(policy_hidden, ref_hidden, mix_num, mix_den, policy_unembed, ref_unembed):
    policy_logits = jnp.dot(policy_hidden, policy_unembed, preferred_element_type=jnp.float32)
    ref_logits = jnp.dot(ref_hidden, ref_unembed, preferred_element_type=jnp.float32)
    beta = (mix_num.astype(jnp.float32) / mix_den.astype(jnp.float32))[:, None]
    mixed = (1.0 - beta) * policy_logits + beta * ref_logits
    top = jnp.max(mixed, axis=1, keepdims=True)
    total = jnp.sum(jnp.exp(mixed - top), axis=1, keepdims=True)
    return mixed - top - jnp.log(total)
```

```python
import jax
import jax.numpy as jnp
from jax import lax
from jax.sharding import PartitionSpec as P

AXES = ("vrow", "vcol")
PART1 = 96


def dotf(a, b):
    return jnp.dot(a, b, preferred_element_type=jnp.float32)


def make_body(rows_of, cols_of):
    chips = cols_of // 2

    def route(move):
        return [
            (r * cols_of + c, (lambda t: t[0] * cols_of + t[1])(move(r, c)))
            for r in range(rows_of)
            for c in range(cols_of)
        ]

    over_core = route(lambda r, c: (r, c ^ 1))
    over_y = route(lambda r, c: (r ^ 1, c))
    over_z = route(lambda r, c: (r ^ 2, c))

    def over_x(step):
        return route(lambda r, c: (r, (c - 2 * step) % cols_of))

    def send(value, pairs):
        return lax.ppermute(value, AXES, pairs)

    def body(policy_hidden, ref_hidden, mix_num, mix_den, policy_unembed, ref_unembed):
        batch, feats = policy_hidden.shape
        vocab = policy_unembed.shape[1]
        hidden = (policy_hidden, ref_hidden)
        unembed = (policy_unembed, ref_unembed)
        quarter = batch // 4
        first = quarter * PART1 // 256
        second = quarter - first
        col = lax.axis_index("vcol")
        core = col % 2
        chip = col // 2
        me = lax.axis_index("vrow") % 4
        beta = (mix_num.astype(jnp.float32) / mix_den.astype(jnp.float32))[:, None]

        def rows(value, j, lo, n):
            return lax.dynamic_slice_in_dim(value, (me ^ j) * quarter + lo, n, 0)

        def columns(weight, shard):
            return lax.dynamic_slice_in_dim(weight, shard * feats, feats, 0)

        steps = range(1, chips)
        x1 = {d: [send(rows(h, 0, 0, first), over_x(d)) for h in hidden] for d in steps}
        x2 = {d: [send(rows(h, 0, first, second), over_x(d)) for h in hidden] for d in steps}
        xd = {d: [send(rows(h, 3, first, second), over_x(d)) for h in hidden] for d in steps}

        shards = [((chip + d) % chips) * 2 for d in range(chips)]
        other = [[send(columns(w, s + 1 - core), over_core) for w in unembed] for s in shards]
        own = [[columns(w, s + core) for w in unembed] for s in shards]

        y1 = {d: [send(v, over_y) for v in x1[d]] for d in steps}
        z1 = {d: [send(v, over_z) for v in x1[d]] for d in steps}
        d1 = {d: [send(z1[d][0], over_y), send(y1[d][1], over_z)] for d in steps}
        y2 = {d: [send(v, over_y) for v in x2[d]] for d in steps}
        z2 = {d: [send(v, over_z) for v in x2[d]] for d in steps}

        def mix(b, policy, ref):
            return (1.0 - b) * policy + b * ref

        def local(weights):
            return mix(beta, dotf(hidden[0], weights[0]), dotf(hidden[1], weights[1]))

        near = (local(own[0]), local(other[0]))
        early = [(0, 0, first, x1), (0, first, second, x2), (1, 0, first, y1), (2, 0, first, z1), (3, 0, first, d1), (3, first, second, xd)]
        late = [(1, first, second, y2), (2, first, second, z2)]

        def logits(pieces):
            pick = lambda value: jnp.concatenate([rows(value, j, lo, n) for j, lo, n, _ in pieces], axis=0)
            b = pick(beta)
            out = []
            for side, weights in ((0, own), (1, other)):
                total = pick(near[side])
                for d in steps:
                    got = [jnp.concatenate([p[3][d][m] for p in pieces], axis=0) for m in range(2)]
                    total = total + mix(b, dotf(got[0], weights[d][0]), dotf(got[1], weights[d][1]))
                out.append(total)
            return out[0] + send(out[1], over_core)

        groups = [(early, logits(early)), (late, logits(late))]
        block = {}
        for pieces, value in groups:
            at = 0
            for j, lo, n, _ in pieces:
                block[j, lo] = value[at : at + n]
                at += n
        by_offset = jnp.stack([jnp.concatenate([block[j, 0], block[j, first]], axis=0) for j in range(4)])
        mixed = jnp.concatenate([lax.dynamic_index_in_dim(by_offset, me ^ q, 0, keepdims=False) for q in range(4)], axis=0)

        top = jnp.max(mixed, axis=1)
        total = jnp.sum(jnp.exp(mixed - top[:, None]), axis=1)
        part = top + jnp.log(total)
        n_dev = rows_of * cols_of
        spread = jnp.broadcast_to(part.reshape(1, 8, batch // 8), (n_dev, 8, batch // 8))
        parts = lax.all_to_all(spread, AXES, 0, 0).reshape(n_dev, batch)
        high = jnp.max(parts, axis=0)
        lse = high + jnp.log(jnp.sum(jnp.exp(parts - high), axis=0))
        return mixed - lse[:, None]

    return body


def solution(mesh):
    return jax.shard_map(
        make_body(mesh.shape["vrow"], mesh.shape["vcol"]),
        mesh=mesh,
        in_specs=(
            P(None, "vcol"),
            P(None, "vcol"),
            P(),
            P(),
            P(None, ("vrow", "vcol")),
            P(None, ("vrow", "vcol")),
        ),
        out_specs=P(None, ("vrow", "vcol")),
        check_vma=False,
    )
```
